32 devices in a mesh: ctx: 4 (over x, core), exp: 8 (over z, y).
Axes of the slice: x: 2, y: 2, z: 4, core: 2. Of those that a mesh axis runs over, the one named last changes fastest.
Arguments:
- q_nope: bfloat16 [128, 128, 512], P('ctx', 'exp'), may hold values from -72 to 72
- q_rope: bfloat16 [128, 8192], P('ctx', 'exp'), may hold values from -6 to 6
- cache_keys: bfloat16 [576, 512], P(None, 'ctx'), may hold values from -6 to 6
- fresh_keys: bfloat16 [576, 128], P(None, 'ctx'), may hold values from -6 to 6
- block_order: int32 [8], replicated, may hold values from 0 to 7, each once
- w_uv: bfloat16 [128, 512, 128], P('exp'), may hold values from -0.25 to 0.25
- w_out: bfloat16 [16384, 7168], P('exp', 'ctx'), may hold values from -0.046875 to 0.046875
- residual: bfloat16 [128, 7168], P(('ctx', 'exp')), may hold values from -6 to 6
- norm_gain: float32 [7168], replicated, may hold values from 0.5 to 1.5
- router_weight: bfloat16 [7168, 16], replicated, may hold values from -0.0625 to 0.0625
- expert_ids: int32 [128, 8], P(('ctx', 'exp')), may hold values from 0 to 15, all different within a row; in each aligned block of 4 rows (0 to 3, 4 to 7, ...) at most 3 rows name the same one
- w_gate: bfloat16 [16, 7168, 2048], P('exp', None, 'ctx'), may hold values from -0.0625 to 0.0625
- w_up: bfloat16 [16, 7168, 2048], P('exp', None, 'ctx'), may hold values from -0.0625 to 0.0625
- w_down: bfloat16 [16, 2048, 7168], P('exp', 'ctx'), may hold values from -0.125 to 0.125
Outputs:
- layer_out: bfloat16 [128, 7168], P(('ctx', 'exp'))
The draws below stay inside these ranges and needn't reach their ends.
Inputs may be any that keep to these rules, and one draw needn't show every extreme that they name: A permutation: block j of the new tokens (16 rows) sits at positions 512 + block_order[j] * 16 onward. `expert_ids`: each row names 8 different experts; the 4 rows of one device name no expert more than 3 times, and in some aligned block one expert exactly 3 times.
All inputs are finite; a program needn't handle non-finite values.
Results may differ from the reference program's by a relative error of at most 0.012.
Values may be sent and summed in bfloat16 or wider, within the bound.
No kernel may reach another device: no remote copies, remote signals or barrier semaphores. Data moves between devices by JAX's collectives and lax.ppermute only.
A program may use at most 128 MiB of HBM per device.

```python
import math
import jax
import jax.numpy as jnp
import numpy as np
from jax import lax

D = 7168
HEADS = 128
LAT = 512
ROPE = 64
QKD = 192
VHD = 128
FF = 2048
TOP = 8
EXPERTS = 16
TOK_DEV = 4
KD = 576
FFS = 512
CAP = 3
BLK = 16
NBLK = 8
NEWTOK = 128
CACHE = 512


def latent_cache(key):
    baseline = jax.random.normal(jax.random.fold_in(key, 101), (KD, CACHE), jnp.float32)
    return jnp.clip(baseline, -6.0, 6.0)


def draw_cache_keys(key, part):
    return latent_cache(key).astype(jnp.bfloat16)


def draw_q_nope(key, part):
    queries = jnp.clip(jax.random.normal(jax.random.fold_in(key, 202), (NEWTOK, HEADS, LAT), jnp.float32), -6.0, 6.0)
    return queries.astype(jnp.bfloat16)


def steps_of(rng, dims, cuts, low, top_value):
    loudness = 1.0
    for position, parts in cuts:
        steps = jax.random.uniform(jax.random.fold_in(jax.random.fold_in(rng, 6), position), (parts,), jnp.float32, low / len(cuts), top_value / len(cuts))
        loudness = loudness * jnp.repeat(jnp.exp(steps), dims[position] // parts).reshape((-1,) + (1,) * (len(dims) - 1 - position))
    return loudness


def shared_out(own_key, own, number, rows, amount, top, limit, skew):
    sequence = jax.random.permutation(own_key, amount)
    crowded, common = load_shares(amount, rows * top, limit, skew, True), load_shares(amount, rows * top, limit, skew, False)
    places = jnp.arange(amount)

    def named(tallies, rotation):
        used = int((tallies > 0).sum())
        fixed = max(1, used // 4)
        moved = fixed + (places - fixed + rotation * (used - fixed)) % max(1, amount - fixed)
        return jnp.zeros((amount,), jnp.int32).at[sequence[jnp.where(places < fixed, places, moved)]].set(jnp.asarray(tallies, jnp.int32))

    tallies = jnp.where(number % 4 == 0, named(crowded, number // 4), named(common, number - number // 4 - 1))
    mixed = jax.random.permutation(jax.random.fold_in(own, 3), amount)
    source_of, sink = mixed[0:amount // 2 * 2:2], mixed[1:amount // 2 * 2:2]
    room = jnp.minimum(tallies[source_of] - 1, limit - tallies[sink]) // 2
    room = jnp.where((source_of == sequence[0]) | (sink == sequence[0]) | (tallies[sink] == 0), 0, jnp.maximum(room, 0))
    moved = jax.random.randint(jax.random.fold_in(own, 4), (amount // 2,), 0, 1 << 20) % (room + 1)
    tallies = tallies.at[source_of].add(-moved).at[sink].add(moved)
    items = jnp.searchsorted(jnp.cumsum(tallies), jnp.arange(rows * top), side="right").astype(jnp.int32)
    table = items.reshape(top, rows).T
    table = table[jax.random.permutation(jax.random.fold_in(own, 1), rows)]
    rotation = jax.random.randint(jax.random.fold_in(own, 2), (rows, 1), 0, top)
    return jnp.take_along_axis(table, (jnp.arange(top)[None, :] + rotation) % top, axis=1)


def load_shares(count, total, bound, slope, full):
    loads = [(1 << 20) // math.isqrt(grade ** slope) + 1 for grade in range(1, count + 1)]
    largest = bound if full else min(bound, max(-(-total // count), total * loads[0] // sum(loads)))
    least = 1 if total - largest >= count - 1 else 0
    given, spare = [largest] + [least] * (count - 1), total - largest - least * (count - 1)
    while spare > 0:
        candidates = [i for i in range(1, count) if given[i] < largest] or [i for i in range(1, count) if given[i] < bound]
        pool, remaining = sum([loads[i] for i in candidates]), spare
        for i in candidates:
            extra = min(bound - given[i], max(1, remaining * loads[i] // pool), spare)
            given[i] = given[i] + extra
            spare = spare - extra
    return np.array(given)


def centred(stream_key, dims, width, most, cuts=(), kind=jnp.bfloat16):
    values = jax.random.normal(stream_key, dims, jnp.float32) * width
    if len(cuts) > 0:
        values = steps_of(stream_key, dims, cuts, -0.22, 0.18) * values
    return jnp.clip(values, min=-most, max=most).astype(kind)


def setup_inputs(seed: int = 0) -> dict:
    key_of = jax.random.split(jax.random.key(seed), 15)
    q_nope = draw_q_nope(jax.random.fold_in(key_of[14], 71), 0)
    q_rope = centred(key_of[1], (NEWTOK, HEADS * ROPE), 1.0, 6.0, ((0, 4), (1, 8)))
    cache_keys = draw_cache_keys(jax.random.fold_in(key_of[14], 71), 0)
    fresh_keys = centred(key_of[3], (KD, NEWTOK), 1.0, 6.0, ((1, 4),))
    block_order = jax.random.permutation(key_of[4], NBLK).astype(jnp.int32)
    w_uv = centred(key_of[5], (HEADS, LAT, VHD), LAT ** -0.5, 0.25, ((0, 8),))
    w_out = centred(key_of[6], (HEADS * VHD, D), (HEADS * VHD) ** -0.5, 0.046875, ((0, 8), (1, 4)))
    residual = centred(key_of[7], (NEWTOK, D), 1.0, 6.0, ((0, 32),))
    norm_gain = jnp.clip(1.0 + 0.1 * jax.random.normal(key_of[8], (D,), jnp.float32), 0.5, 1.5)
    router_weight = centred(key_of[9], (D, EXPERTS), D ** -0.5, 0.0625)
    expert_ids_keys = jax.random.split(jax.random.fold_in(key_of[10], 1), NEWTOK // TOK_DEV)
    expert_ids_turns = jax.random.permutation(jax.random.fold_in(key_of[10], 3), NEWTOK // TOK_DEV)
    expert_ids = jax.vmap(lambda own, number: shared_out(jax.random.fold_in(key_of[10], 2), own, number, TOK_DEV, EXPERTS, TOP, CAP, 2))(expert_ids_keys, expert_ids_turns).reshape((NEWTOK, TOP))
    w_gate = centred(key_of[11], (EXPERTS, D, FF), D ** -0.5, 0.0625, ((0, 8), (2, 4)))
    w_up = centred(key_of[12], (EXPERTS, D, FF), D ** -0.5, 0.0625, ((0, 8), (2, 4)))
    w_down = centred(key_of[13], (EXPERTS, FF, D), FF ** -0.5, 0.125, ((0, 8), (1, 4)))
    return dict(q_nope=q_nope, q_rope=q_rope, cache_keys=cache_keys, fresh_keys=fresh_keys, block_order=block_order, w_uv=w_uv, w_out=w_out, residual=residual, norm_gain=norm_gain, router_weight=router_weight, expert_ids=expert_ids, w_gate=w_gate, w_up=w_up, w_down=w_down)


ROUTE_SCALE = 2.5
NORM_EPS = 1e-06

def block_position(row_index, block_order):
    blocks = row_index // BLK
    lookup = blocks[:, None] == jnp.arange(NBLK, dtype=jnp.int32)[None, :]
    leading = lax.optimization_barrier(jnp.sum(jnp.where(lookup, block_order[None, :], 0), axis=1))
    return (leading * BLK + row_index % BLK).astype(jnp.int32)

def reference(q_nope, q_rope, cache_keys, fresh_keys, block_order, w_uv, w_out, residual, norm_gain, router_weight, expert_ids, w_gate, w_up, w_down):
    keys = jnp.concatenate([cache_keys, fresh_keys], axis=1)
    query_pos = block_position(jnp.arange(NEWTOK, dtype=jnp.int32), block_order)
    key_pos = jnp.concatenate([jnp.full((CACHE,), -1, jnp.int32), query_pos])
    visible = key_pos[None, :] <= query_pos[:, None]
    scale = 1.0 / math.sqrt(QKD)
    latent_keys = keys[:LAT]
    rotary_keys = keys[LAT:]

    def one_head(inputs):
        query_lat, query_pe, w_head = inputs
        first_dot = jnp.dot(query_lat, latent_keys, preferred_element_type=jnp.float32)
        second_dot = jnp.dot(query_pe, rotary_keys, preferred_element_type=jnp.float32)
        scores = jnp.where(visible, (first_dot + second_dot) * scale, -jnp.inf)
        row_max = lax.optimization_barrier(jnp.max(scores, axis=1, keepdims=True))
        exponent = jnp.exp(scores - row_max)
        row_sum = lax.optimization_barrier(jnp.sum(exponent, axis=1, keepdims=True))
        latent = lax.dot_general(exponent.astype(jnp.bfloat16), latent_keys, (((1,), (1,)), ((), ())), preferred_element_type=jnp.float32) / row_sum
        return jnp.dot(latent, w_head.astype(jnp.float32), precision=lax.Precision.HIGHEST).astype(jnp.bfloat16)
    head_inputs = (jnp.transpose(q_nope, (1, 0, 2)), jnp.transpose(q_rope.reshape(NEWTOK, HEADS, ROPE), (1, 0, 2)), w_uv)
    head_out = lax.map(one_head, head_inputs)
    head_out = jnp.transpose(head_out, (1, 0, 2)).reshape(NEWTOK, HEADS * VHD)
    attention = jnp.dot(head_out, w_out, preferred_element_type=jnp.float32).astype(jnp.bfloat16)
    hidden = residual.astype(jnp.float32) + attention.astype(jnp.float32)
    mean_square = lax.optimization_barrier(jnp.mean(hidden * hidden, axis=1, keepdims=True))
    normed = (hidden * lax.rsqrt(mean_square + NORM_EPS) * norm_gain).astype(jnp.bfloat16)
    affinity = jax.nn.sigmoid(jnp.dot(normed, router_weight, preferred_element_type=jnp.float32))
    chosen = jnp.take_along_axis(affinity, expert_ids, axis=1)
    route = ROUTE_SCALE * chosen / lax.optimization_barrier(jnp.sum(chosen, axis=1, keepdims=True))
    onehot = expert_ids[:, :, None] == jnp.arange(EXPERTS, dtype=jnp.int32)[None, None, :]
    mixing = lax.optimization_barrier(jnp.sum(jnp.where(onehot, route[:, :, None], 0.0), axis=1))

    def one_expert(running, inputs):
        gate_matrix, up_matrix, down_matrix, mix_column = inputs
        gate = jnp.dot(normed, gate_matrix, preferred_element_type=jnp.float32)
        upward = jnp.dot(normed, up_matrix, preferred_element_type=jnp.float32)
        act = (jax.nn.silu(gate) * upward).astype(jnp.bfloat16)
        act_blocks = jnp.transpose(act.reshape(NEWTOK, FF // FFS, FFS), (1, 0, 2))
        down_blocks = down_matrix.reshape(FF // FFS, FFS, D)

        def add_block(accum, pair):
            block_out = jnp.dot(pair[0], pair[1], preferred_element_type=jnp.float32).astype(jnp.bfloat16)
            block_out = lax.optimization_barrier(block_out)
            return (accum + block_out.astype(jnp.float32), None)
        summed, ignored = lax.scan(add_block, jnp.zeros((NEWTOK, D), jnp.float32), (act_blocks, down_blocks))
        expert_out = lax.optimization_barrier(summed.astype(jnp.bfloat16)).astype(jnp.float32)
        return (running + mix_column[:, None] * expert_out, None)
    mixture, ignored = lax.scan(one_expert, jnp.zeros((NEWTOK, D), jnp.float32), (w_gate, w_up, w_down, mixing.T))
    return (hidden + mixture).astype(jnp.bfloat16)
```

```python
import math

import jax
import jax.numpy as jnp
from jax import lax
from jax.experimental import pallas as pl
from jax.experimental.pallas import tpu as pltpu
from jax.sharding import PartitionSpec as P


QKD = 192
ROUTE_SCALE = 2.5
NORM_EPS = 1e-06
EXTRA = 128
IDS = 16
BF = jnp.bfloat16
F32 = jnp.float32
I32 = jnp.int32
NT = (((1,), (1,)), ((), ()))


def bits_of(count):
    masks = []
    bit = 1
    while bit < count:
        masks.append(bit)
        bit *= 2
    return masks


def subsets(masks):
    out = [0]
    for m in masks:
        out = out + [s | m for s in out]
    return out


def held(x):
    return pltpu.with_memory_space_constraint(x, pltpu.VMEM)


def dot(a, b):
    return jnp.dot(a, b, preferred_element_type=F32)


def dot_t(a, b):
    return lax.dot_general(a, b, NT, preferred_element_type=F32)


def call(kernel, outs, args, specs, limit, flops, loads=(), scratch=()):
    shapes = [jax.ShapeDtypeStruct(s, d) for s, d in outs]
    shapes += [pltpu.VMEM(s, BF) for s in loads]
    args = [
        pltpu.with_memory_space_constraint(a, pltpu.HBM) if s == pltpu.HBM else a
        for a, s in zip(args, specs)
    ]
    got = pl.pallas_call(
        kernel,
        out_shape=tuple(shapes),
        in_specs=[pl.BlockSpec(memory_space=s) for s in specs],
        out_specs=tuple(pl.BlockSpec(memory_space=pltpu.VMEM) for _ in shapes),
        scratch_shapes=list(scratch),
        compiler_params=pltpu.CompilerParams(vmem_limit_bytes=limit << 20),
        cost_estimate=pl.CostEstimate(flops=flops, bytes_accessed=0, transcendentals=0),
    )(*args)
    return list(got)


def pick(index, table):
    out = jnp.zeros(index.shape, I32)
    for i, v in enumerate(table):
        out = jnp.where(index == i, v, out)
    return out


def attend(meta, q, qr, kc, kf, w_uv, w_out, korder, block_rows):
    nctx = len(kc)
    kd, cache_len = kc[0].shape
    rows = kf[0].shape[0]
    heads, lat, vh = w_uv.shape
    group = max(1, 128 // rows)
    nblk = meta.shape[0] - 2

    def kernel(*refs):
        idx_ref, q_ref, qr_ref = refs[:3]
        kc_ref = refs[3 : 3 + nctx]
        kf_ref = refs[3 + nctx : 3 + 2 * nctx]
        w_hbm, wo_hbm, out_ref, wo_ref, w_ref, sems = refs[3 + 2 * nctx :]
        load = pltpu.make_async_copy(w_hbm, w_ref, sems.at[0])
        load.start()
        load_out = pltpu.make_async_copy(wo_hbm, wo_ref, sems.at[1])
        load_out.start()
        c = idx_ref[0]
        starts = [idx_ref[2 + b] * block_rows for b in range(nblk)]

        def position(grow):
            return pick(grow // block_rows, starts) + grow % block_rows

        kfa = jnp.concatenate([k[...] for k in kf_ref], axis=0)
        kca = jnp.concatenate([k[...] for k in kc_ref], axis=1)
        col = lax.broadcasted_iota(I32, (1, nctx * rows), 1)
        owner = pick(col // rows, [c ^ k for k in korder])
        kpos = position(owner * rows + col % rows)
        row = lax.broadcasted_iota(I32, (group * rows, 1), 0)
        qpos = position(c * rows + row % rows)
        visible = kpos <= qpos
        scale = 1.0 / math.sqrt(QKD)
        for g in range(heads // group):
            lo = g * group * rows
            qb = q_ref[lo : lo + group * rows, :]
            rb = qr_ref[lo : lo + group * rows, :]
            sc = (dot(qb, kca[:lat]) + dot(rb, kca[lat:])) * scale
            sf = (dot_t(qb, kfa[:, :lat]) + dot_t(rb, kfa[:, lat:])) * scale
            sf = jnp.where(visible, sf, -jnp.inf)
            top = jnp.maximum(
                jnp.max(sc, axis=1, keepdims=True), jnp.max(sf, axis=1, keepdims=True)
            )
            pc = jnp.exp(sc - top)
            pf = jnp.exp(sf - top)
            total = jnp.sum(pc, axis=1, keepdims=True) + jnp.sum(pf, axis=1, keepdims=True)
            acc = dot_t(pc.astype(BF), kca[:lat]) + dot(pf.astype(BF), kfa[:, :lat])
            acc = acc / total
            hi = acc.astype(BF)
            low = (acc - hi.astype(F32)).astype(BF)
            if g == 0:
                load.wait()
            for h in range(group):
                w = w_ref[g * group + h]
                a = h * rows
                v = dot(hi[a : a + rows], w) + dot(low[a : a + rows], w)
                n = (g * group + h) * vh
                out_ref[:, n : n + vh] = v.astype(BF)
        load_out.wait()

    specs = (pltpu.SMEM,) + (pltpu.VMEM,) * (2 + 2 * nctx) + (pltpu.HBM,) * 2
    flops = 2 * heads * rows * nctx * (cache_len + rows) * (kd + lat)
    return call(
        kernel,
        [((rows, heads * vh), BF)],
        (meta, q, qr, *kc, *kf, w_uv, w_out),
        specs,
        16,
        flops,
        [w_out.shape],
        [pltpu.VMEM(w_uv.shape, BF), pltpu.SemaphoreType.DMA((2,))],
    )


def project(idx, hg, w_out, korder, emasks, tok):
    nctx = len(hg)
    rows, width = hg[0].shape
    total = nctx * rows
    cols = w_out.shape[1]

    def kernel(idx_ref, *refs):
        hg_ref = refs[:nctx]
        w_ref, send_ref, keep_ref = refs[nctx:]
        c = idx_ref[0]
        e = idx_ref[1]
        r = lax.broadcasted_iota(I32, (total, 1), 0)
        place = [0] * nctx
        for i, k in enumerate(korder):
            place[k] = i
        kp = jnp.zeros(r.shape, I32)
        rel = (r // tok) % nctx
        for k in range(nctx):
            kp = jnp.where(rel == (c ^ k), place[k], kp)
        j = pick(r // (nctx * tok), [e ^ m for m in emasks])
        src = kp * rows + j * tok + r % tok
        perm = (src == lax.broadcasted_iota(I32, (total, total), 1)).astype(F32).astype(BF)
        lhs = dot(perm, jnp.concatenate([h[...] for h in hg_ref], axis=0)).astype(BF)
        half = total // 2
        full = dot(lhs, w_ref[...])
        send_ref[...] = full[half:].astype(BF)
        keep_ref[...] = full[:half]

    return call(
        kernel,
        [((total // 2, cols), BF), ((total // 2, cols), F32)],
        (idx, *hg, held(w_out)),
        (pltpu.SMEM,) + (pltpu.VMEM,) * (nctx + 1),
        12,
        2 * total * width * cols,
    )


def choose(pairs):
    out = None
    for cond, x in pairs:
        x = jnp.where(cond, x, 0.0)
        out = x if out is None else out + x
    return out


def residual_parts(idx, residual, ids, nctx):
    tok, width = residual.shape
    cols = width // nctx
    top = ids.shape[1]

    def kernel(idx_ref, res_ref, ids_ref, *outs):
        c = idx_ref[0]
        lane = lax.broadcasted_iota(I32, (tok, EXTRA), 1)
        side = jnp.zeros((tok, EXTRA), F32)
        for t in range(top):
            side = jnp.where(lane - IDS == ids_ref[:, t : t + 1], 1.0, side)
        res = res_ref[...].astype(F32)
        for k in range(nctx):
            outs[k][:, :cols] = choose(
                [((c ^ k) == j, res[:, j * cols : (j + 1) * cols]) for j in range(nctx)]
            ).astype(BF)
            outs[k][:, cols:] = side.astype(BF)

    return call(
        kernel,
        [((tok, cols + EXTRA), BF)] * nctx,
        (idx, residual, ids),
        (pltpu.SMEM, pltpu.VMEM, pltpu.VMEM),
        4,
        1 << 28,
    )


def one_hot_rows(out_rows, in_rows, tok, shift):
    r = lax.broadcasted_iota(I32, (out_rows, in_rows), 0)
    q = lax.broadcasted_iota(I32, (out_rows, in_rows), 1)
    return ((r == q + shift * tok)).astype(F32).astype(BF)


def merge(idx, parts, own, got, gain, tok):
    nctx = len(parts)
    blk, cols = own.shape
    hc = cols // 2
    n = len(got)

    def kernel(idx_ref, *refs):
        c = idx_ref[0]
        prefs = refs[:nctx]
        own_ref = refs[nctx]
        grefs = refs[nctx + 1 : nctx + 1 + n]
        gain_ref, sx_ref, att_ref = refs[nctx + 1 + n :]
        att = own_ref[...]
        for g in grefs:
            att = att + g[...].astype(F32)
        att = att.astype(BF)
        att_ref[...] = att
        res = None
        for k in range(nctx):
            part = dot(one_hot_rows(blk, tok, tok, c ^ k), prefs[k][...])
            res = part if res is None else res + part
        hidden = res[:, :cols] + att.astype(F32)
        ssq = jnp.sum(hidden * hidden, axis=1, keepdims=True)
        gain = choose(
            [(c == j, gain_ref[:, j * cols : (j + 1) * cols]) for j in range(nctx)]
        )
        scaled = hidden * gain
        hi = ssq.astype(BF).astype(F32)
        mid = (ssq - hi).astype(BF).astype(F32)
        low = ssq - hi - mid
        extra = res[:, cols:]
        lane = lax.broadcasted_iota(I32, extra.shape, 1)
        extra = jnp.where(lane == 0, hi, jnp.where(lane == 1, mid, extra))
        extra = jnp.where(lane == 2, low, extra)
        sx_ref[:, :hc] = scaled[:, :hc].astype(BF)
        sx_ref[:, hc : hc + EXTRA] = extra.astype(BF)
        sx_ref[:, hc + EXTRA :] = scaled[:, hc:].astype(BF)

    return call(
        kernel,
        [((blk, cols + EXTRA), BF), ((blk, cols), BF)],
        (idx, *parts, own, *got, gain),
        (pltpu.SMEM,) + (pltpu.VMEM,) * (nctx + n + 2),
        4,
        1 << 28,
    )


def attention_parts(idx, att, nctx, tok):
    cols = att.shape[1]

    def kernel(idx_ref, att_ref, *outs):
        c = idx_ref[0]
        r = lax.broadcasted_iota(I32, (tok, nctx * tok), 0)
        q = lax.broadcasted_iota(I32, (tok, nctx * tok), 1)
        for k in range(nctx):
            pickr = (q == r + (c ^ k) * tok).astype(F32).astype(BF)
            outs[k][...] = dot(pickr, att_ref[...]).astype(BF)

    return call(
        kernel,
        [((tok, cols), BF)] * nctx,
        (idx, att),
        (pltpu.SMEM, pltpu.VMEM),
        4,
        1 << 28,
    )


def finalize(idx, residual, parts, own, got):
    nctx = len(parts)
    tok, width = residual.shape
    cols = width // nctx
    n = len(got)

    def kernel(idx_ref, res_ref, *refs):
        c = idx_ref[0]
        prefs = [p[...].astype(F32) for p in refs[:nctx]]
        own_ref = refs[nctx]
        grefs = refs[nctx + 1 : nctx + 1 + n]
        out_ref = refs[nctx + 1 + n]
        for j in range(nctx):
            a, b = j * cols, (j + 1) * cols
            att = choose([((c ^ k) == j, prefs[k]) for k in range(nctx)])
            mix = own_ref[:, a:b]
            for g in grefs:
                mix = mix + g[:, a:b].astype(F32)
            out_ref[:, a:b] = (res_ref[:, a:b].astype(F32) + att + mix).astype(BF)

    return call(
        kernel,
        [((tok, width), BF)],
        (idx, residual, *parts, own, *got),
        (pltpu.SMEM,) + (pltpu.VMEM,) * (nctx + n + 2),
        4,
        1 << 28,
    )[0]


class Chunk:
    def __init__(self, pieces, mask, half):
        self.pieces = pieces
        self.mask = mask
        self.half = half


def grab(arrays):
    n = len(arrays)

    def kernel(*refs):
        tok_ref = refs[n]
        sems = refs[2 * n + 1]
        copies = []
        for i in range(n):
            copies.append(pltpu.make_async_copy(refs[i], refs[n + 1 + i], sems.at[i]))
            copies[-1].start()
        tok_ref[...] = jnp.zeros(tok_ref.shape, F32)
        for cp in copies:
            cp.wait()

    done, *got = call(
        kernel,
        [((8, 128), F32)],
        tuple(arrays),
        (pltpu.HBM,) * n,
        1,
        1 << 30,
        [a.shape for a in arrays],
        [pltpu.SemaphoreType.DMA((n,))],
    )
    return done, got


def fetch(idx, blocks, w_gate, w_up, hc):
    local, _, ff = w_gate.shape
    n = len(blocks)

    def kernel(idx_ref, wg_ref, wu_ref, tok_ref, *refs):
        sems = refs[2 * n]
        copies = []
        for i, (mask, half) in enumerate(blocks):
            start = pl.multiple_of(((idx_ref[0] ^ mask) * 2 + half) * hc, 16)
            for j, src in enumerate((wg_ref, wu_ref)):
                cp = pltpu.make_async_copy(
                    src.at[:, pl.ds(start, hc), :], refs[2 * i + j], sems.at[i, j]
                )
                cp.start()
                copies.append(cp)
        tok_ref[...] = jnp.zeros(tok_ref.shape, F32)
        for cp in copies:
            cp.wait()

    shape = (local, hc, ff)
    done, *got = call(
        kernel,
        [((8, 128), F32)],
        (idx, w_gate, w_up),
        (pltpu.SMEM, pltpu.HBM, pltpu.HBM),
        1,
        1 << 30,
        [shape] * (2 * n),
        [pltpu.SemaphoreType.DMA((n, 2))],
    )
    return done, {b: (got[2 * i], got[2 * i + 1]) for i, b in enumerate(blocks)}


def experts(idx, chunks, router, weights, width, carry, finish):
    loaded = [held(w) for ch in chunks for w in weights[ch.mask, ch.half]]
    local, hc, ff = loaded[0].shape
    nw = len(loaded)
    pieces = [p for ch in chunks for p in ch.pieces]
    total = sum(p.shape[0] for p in chunks[0].pieces)
    nexperts = router.shape[1]
    n = len(pieces)
    ncarry = len(carry)

    def kernel(*refs):
        idx_ref = refs[0]
        prefs = refs[1 : 1 + n]
        r_ref = refs[1 + n]
        wrefs = refs[2 + n : 2 + n + nw]
        crefs = refs[2 + n + nw : 2 + n + nw + ncarry]
        outs = refs[2 + n + nw + ncarry :]
        c = idx_ref[0]
        xs = []
        at = 0
        logit = crefs[2][...] if ncarry else jnp.zeros((total, nexperts), F32)
        ssum = crefs[3][...] if ncarry else jnp.zeros((total, 1), F32)
        for ch in chunks:
            parts = [prefs[at + i][...] for i in range(len(ch.pieces))]
            at += len(parts)
            x = parts[0] if len(parts) == 1 else jnp.concatenate(parts, axis=0)
            block = (c ^ ch.mask) * 2 + ch.half
            if ch.half == 0:
                extra = x[:, hc : hc + EXTRA].astype(F32)
                lane = lax.broadcasted_iota(I32, extra.shape, 1)
                ssum = ssum + jnp.sum(jnp.where(lane < 3, extra, 0.0), axis=1, keepdims=True)
                chosen = extra[:, IDS : IDS + nexperts]
            x = x[:, :hc]
            xs.append(x)
            logit = logit + dot_t(x, r_ref[block])
        if finish is None:
            for e in range(local):
                for c_i in (0, 1):
                    acc = crefs[c_i][e] if ncarry else None
                    for i, x in enumerate(xs):
                        part = dot(x, wrefs[2 * i + c_i][e])
                        acc = part if acc is None else acc + part
                    outs[c_i][e] = acc
            outs[2][...] = logit
            outs[3][...] = ssum
            return
        scale = lax.rsqrt(ssum / width + NORM_EPS)
        affinity = jax.nn.sigmoid(logit * scale) * chosen
        mixing = ROUTE_SCALE * affinity / jnp.sum(affinity, axis=1, keepdims=True)
        lane = lax.broadcasted_iota(I32, mixing.shape, 1)
        acts = []
        for e in range(local):
            vals = []
            for c_i in (0, 1):
                acc = crefs[c_i][e]
                for i, x in enumerate(xs):
                    acc = acc + dot(x, wrefs[2 * i + c_i][e])
                vals.append(acc * scale)
            mine = idx_ref[1] * local + e
            mix = jnp.sum(jnp.where(lane == mine, mixing, 0.0), axis=1, keepdims=True)
            acts.append((jax.nn.silu(vals[0]) * vals[1] * mix).astype(BF))
        act = jnp.concatenate(acts, axis=1)
        nctx, tok, order_in, plans = finish
        r = lax.broadcasted_iota(I32, (total, 1), 0)
        for plan, out_ref in zip(plans, outs):
            pos = r // tok
            cm = pick(pos, [a for a, _ in plan])
            where_in = [order_in.index(b) for _, b in plan]
            p = pick(pos, where_in)
            src = (p * nctx + (c ^ cm)) * tok + r % tok
            perm = (src == lax.broadcasted_iota(I32, (total, total), 1)).astype(F32).astype(BF)
            out_ref[...] = dot(perm, act).astype(BF)

    acc_shape = (local, total, ff)
    if finish is None:
        outs = [(acc_shape, F32), (acc_shape, F32), ((total, nexperts), F32), ((total, 1), F32)]
    else:
        outs = [((total, local * ff), BF), ((total, local * ff), BF)]
    args = (idx, *pieces, router, *loaded, *carry)
    specs = (pltpu.SMEM,) + (pltpu.VMEM,) * (len(args) - 1)
    flops = len(chunks) * 4 * total * hc * ff * local
    return call(kernel, outs, args, specs, 8, flops)


def down(lhs, w_down, lo):
    total = lhs.shape[0]
    local, ff, width = w_down.shape
    hw = width // 2

    def kernel(x_ref, w_ref, send_ref, keep_ref):
        half = total // 2
        step = hw // 4
        for i in range(4):
            acc = None
            for e in range(local):
                part = dot(
                    x_ref[:, e * ff : (e + 1) * ff],
                    w_ref[e, :, lo + i * step : lo + (i + 1) * step],
                )
                acc = part if acc is None else acc + part
            send_ref[:, i * step : (i + 1) * step] = acc[half:].astype(BF)
            keep_ref[:, i * step : (i + 1) * step] = acc[:half]

    return call(
        kernel,
        [((total // 2, hw), BF), ((total // 2, hw), F32)],
        (lhs, held(w_down)),
        (pltpu.VMEM, pltpu.VMEM),
        8,
        2 * total * local * ff * hw,
    )


def body(
    q_nope,
    q_rope,
    cache_keys,
    fresh_keys,
    block_order,
    w_uv,
    w_out,
    residual,
    norm_gain,
    router_weight,
    expert_ids,
    w_gate,
    w_up,
    w_down,
):
    nctx = lax.axis_size("ctx")
    nexp = lax.axis_size("exp")
    c = lax.axis_index("ctx")
    e = lax.axis_index("exp")
    idx = jnp.stack([c, e]).astype(I32)
    cmasks = bits_of(nctx)
    emasks = bits_of(nexp)
    core, xs = cmasks[0], cmasks[1:]
    ym, zs = emasks[0], emasks[1:]
    zsub = subsets(zs)
    eorder = [y ^ z for y in (0, ym) for z in zsub]

    def swap(x, cm=0, em=0):
        m = cm * nexp + em
        return lax.ppermute(x, ("ctx", "exp"), [(i, i ^ m) for i in range(nctx * nexp)])

    rows_here, heads_here, lat = q_nope.shape
    tok, width = residual.shape
    cols = w_out.shape[1]
    hc = cols // 2
    total_rows = nctx * rows_here
    nexperts = router_weight.shape[1]
    block_rows = total_rows // block_order.shape[0]
    pe = q_rope.shape[1] // heads_here

    def spread(group):
        sets = [[x] for x in group]
        for m in xs:
            sets = [got + [swap(g, cm=m) for g in got] for got in sets]
        return [got + [swap(g, cm=core) for g in got] for got in sets]

    korder = subsets(xs)
    korder = korder + [k ^ core for k in korder]

    kf_own = fresh_keys.T
    kc_v, kf_v = grab((cache_keys, kf_own))[1]
    q = q_nope.transpose(1, 0, 2).reshape(heads_here * rows_here, lat)
    qr = q_rope.reshape(rows_here, heads_here, pe).transpose(1, 0, 2)
    qr = qr.reshape(heads_here * rows_here, pe)
    meta = jnp.concatenate([idx, block_order])
    kc, kf = spread((cache_keys, kf_own))
    kc[0], kf[0] = held(kc_v), held(kf_v)
    head, w_out_v = attend(meta, q, qr, kc, kf, w_uv, w_out, korder, block_rows)

    xorder = subsets(xs)
    nx = len(xorder)
    order = [(m, h) for m in xorder for h in (0, 1)]
    order = order + [(m ^ core, h) for m, h in order]
    count = len(order)
    weights = {}
    for lo, hi in FETCHES:
        part = order[count * lo // 8 : count * hi // 8]
        weights.update(fetch(idx, part, w_gate, w_up, hc)[1])
    down_v = grab((w_down,))[1][0]

    res_got = residual_parts(idx, residual, expert_ids, nctx)
    res_got = [swap(p, cm=k) if k else p for k, p in enumerate(res_got)]

    (hg,) = spread((head,))
    send, keep = project(idx, hg, w_out_v, korder, eorder, tok)

    summed = keep + swap(send, em=ym).astype(F32)
    blk = nctx * tok
    got = [
        swap(summed[i * blk : (i + 1) * blk].astype(BF), em=m)
        for i, m in enumerate(zsub)
        if m
    ]
    sx, att_blk = merge(idx, res_got, summed[:blk], got, norm_gain[None], tok)

    zx = jnp.stack([swap(sx, em=m) if m else sx for m in zsub])
    zx = zx.reshape(len(zsub) * blk, -1)
    za = zx[:, : hc + EXTRA][None]
    zb = zx[:, hc + EXTRA :][None]
    own_a = jnp.concatenate([za, swap(za, em=ym)], axis=1)
    xb = zb
    for m in xs:
        xb = jnp.concatenate([xb, swap(xb, cm=m)], axis=0)
    far_b = swap(xb, em=ym)
    xa = own_a
    for m in xs:
        xa = jnp.concatenate([xa, swap(xa, cm=m)], axis=0)
    own_a_core = swap(own_a, cm=core)
    xb_core = swap(xb, cm=core)
    rest_a = xa[1:]
    rest_a_core = swap(rest_a, cm=core)
    far_b_core = swap(far_b, cm=core)

    router = router_weight.reshape(2 * nctx, hc, nexperts).transpose(0, 2, 1)
    first = [Chunk([own_a[0]], 0, 0)]
    g1 = experts(idx, first, router, weights, width, (), None)
    second = [Chunk([rest_a[i - 1]], xorder[i], 0) for i in range(1, nx)]
    second += [Chunk([xb[i], far_b[i]], xorder[i], 1) for i in range(nx)]
    g2 = experts(idx, second, router, weights, width, g1, None)
    third = [Chunk([own_a_core[0]], core, 0)]
    third += [Chunk([rest_a_core[i - 1]], core ^ xorder[i], 0) for i in range(1, nx)]
    third += [Chunk([xb_core[i], far_b_core[i]], core ^ xorder[i], 1) for i in range(nx)]

    xsub = subsets(xs)
    plan_a = [
        (k ^ x, y ^ z) for k in (0, core) for x in xsub for y in (0, ym) for z in zsub
    ]
    plan_b = [
        (k ^ x, y ^ z) for k in (0, core) for y in (0, ym) for x in xsub for z in zsub
    ]
    steps_a = [(m, 0) for m in reversed(xs)] + [(0, ym)]
    steps_b = [(0, ym)] + [(m, 0) for m in reversed(xs)]
    finish = (nctx, tok, eorder, (plan_a, plan_b))
    lhs_a, lhs_b = experts(idx, third, router, weights, width, g2, finish)

    outs = []
    hw = width // 2
    for lhs, lo, steps in ((lhs_a, 0, steps_a), (lhs_b, hw, steps_b)):
        send, keep = down(lhs, down_v, lo)
        x = keep + swap(send, cm=core).astype(F32)
        for cm, em in steps:
            half = x.shape[0] // 2
            got = swap(x[half:].astype(BF), cm=cm, em=em)
            x = x[:half] + got.astype(F32)
        outs.append(x)

    parts = attention_parts(idx, att_blk, nctx, tok)
    parts = [swap(p, cm=k) if k else p for k, p in enumerate(parts)]

    both = jnp.concatenate(outs, axis=1)
    got = [
        swap(both[i * tok : (i + 1) * tok].astype(BF), em=m)
        for i, m in enumerate(zsub)
        if m
    ]
    return finalize(idx, residual, parts, both[:tok], got)


FETCHES = ((0, 2), (2, 4), (4, 7), (7, 8))


def solution(mesh):
    return jax.shard_map(
        body,
        mesh=mesh,
        in_specs=(
            P("ctx", "exp", None),
            P("ctx", "exp"),
            P(None, "ctx"),
            P(None, "ctx"),
            P(),
            P("exp", None, None),
            P("exp", "ctx"),
            P(("ctx", "exp"), None),
            P(),
            P(),
            P(("ctx", "exp"), None),
            P("exp", None, "ctx"),
            P("exp", None, "ctx"),
            P("exp", "ctx", None),
        ),
        out_specs=P(("ctx", "exp"), None),
        check_vma=False,
    )
```

```python
import math

import jax
import jax.numpy as jnp
from jax import lax
from jax.experimental import pallas as pl
from jax.experimental.pallas import tpu as pltpu
from jax.sharding import PartitionSpec as P


QKD = 192
ROUTE_SCALE = 2.5
NORM_EPS = 1e-06
EXTRA = 128
IDS = 16
GROUP_ROWS = 128
BF = jnp.bfloat16
F32 = jnp.float32
I32 = jnp.int32
NT = (((1,), (1,)), ((), ()))


def bits_of(count):
    masks = []
    bit = 1
    while bit < count:
        masks.append(bit)
        bit *= 2
    return masks


def subsets(masks):
    out = [0]
    for m in masks:
        out = out + [s | m for s in out]
    return out


def held(x):
    return pltpu.with_memory_space_constraint(x, pltpu.VMEM)


def dot(a, b):
    return jnp.dot(a, b, preferred_element_type=F32)


def dot_t(a, b):
    return lax.dot_general(a, b, NT, preferred_element_type=F32)


def call(kernel, outs, args, specs, limit, flops, loads=(), scratch=()):
    shapes = [jax.ShapeDtypeStruct(s, d) for s, d in outs]
    shapes += [pltpu.VMEM(s, BF) for s in loads]
    args = [
        pltpu.with_memory_space_constraint(a, pltpu.HBM) if s == pltpu.HBM else a
        for a, s in zip(args, specs)
    ]
    got = pl.pallas_call(
        kernel,
        out_shape=tuple(shapes),
        in_specs=[pl.BlockSpec(memory_space=s) for s in specs],
        out_specs=tuple(pl.BlockSpec(memory_space=pltpu.VMEM) for _ in shapes),
        scratch_shapes=list(scratch),
        compiler_params=pltpu.CompilerParams(vmem_limit_bytes=limit << 20),
        cost_estimate=pl.CostEstimate(flops=flops, bytes_accessed=0, transcendentals=0),
    )(*args)
    return list(got)


def pick(index, table):
    out = jnp.zeros(index.shape, I32)
    for i, v in enumerate(table):
        out = jnp.where(index == i, v, out)
    return out


def attend(meta, q, qr, kc, kf, w_uv, w_out, korder, block_rows):
    nctx = len(kc)
    kd, cache_len = kc[0].shape
    rows = kf[0].shape[0]
    heads, lat, vh = w_uv.shape
    group = max(1, min(heads, GROUP_ROWS // rows))
    nblk = meta.shape[0] - 2

    def kernel(*refs):
        idx_ref, q_ref, qr_ref = refs[:3]
        kc_ref = refs[3 : 3 + nctx]
        kf_ref = refs[3 + nctx : 3 + 2 * nctx]
        w_ref, wo_hbm, out_ref, wo_ref, sem = refs[3 + 2 * nctx :]
        load = pltpu.make_async_copy(wo_hbm, wo_ref, sem)
        load.start()
        c = idx_ref[0]
        starts = [idx_ref[2 + b] * block_rows for b in range(nblk)]

        def position(grow):
            return pick(grow // block_rows, starts) + grow % block_rows

        kfa = jnp.concatenate([k[...] for k in kf_ref], axis=0)
        kca = jnp.concatenate([k[...] for k in kc_ref], axis=1)
        col = lax.broadcasted_iota(I32, (1, nctx * rows), 1)
        owner = pick(col // rows, [c ^ k for k in korder])
        kpos = position(owner * rows + col % rows)
        row = lax.broadcasted_iota(I32, (group * rows, 1), 0)
        qpos = position(c * rows + row % rows)
        visible = kpos <= qpos
        scale = 1.0 / math.sqrt(QKD)
        for g in range(heads // group):
            lo = g * group * rows
            qb = q_ref[lo : lo + group * rows, :]
            rb = qr_ref[lo : lo + group * rows, :]
            sc = (dot(qb, kca[:lat]) + dot(rb, kca[lat:])) * scale
            sf = (dot_t(qb, kfa[:, :lat]) + dot_t(rb, kfa[:, lat:])) * scale
            sf = jnp.where(visible, sf, -jnp.inf)
            top = jnp.maximum(
                jnp.max(sc, axis=1, keepdims=True), jnp.max(sf, axis=1, keepdims=True)
            )
            pc = jnp.exp(sc - top)
            pf = jnp.exp(sf - top)
            total = jnp.sum(pc, axis=1, keepdims=True) + jnp.sum(pf, axis=1, keepdims=True)
            acc = dot_t(pc.astype(BF), kca[:lat]) + dot(pf.astype(BF), kfa[:, :lat])
            acc = acc / total
            hi = acc.astype(BF)
            low = (acc - hi.astype(F32)).astype(BF)
            for h in range(group):
                w = w_ref[g * group + h]
                a = h * rows
                v = dot(hi[a : a + rows], w) + dot(low[a : a + rows], w)
                n = (g * group + h) * vh
                out_ref[:, n : n + vh] = v.astype(BF)
        load.wait()

    specs = (pltpu.SMEM,) + (pltpu.VMEM,) * (3 + 2 * nctx) + (pltpu.HBM,)
    flops = 2 * heads * rows * nctx * (cache_len + rows) * (kd + lat)
    return call(
        kernel,
        [((rows, heads * vh), BF)],
        (meta, q, qr, *kc, *kf, held(w_uv), w_out),
        specs,
        16,
        flops,
        [w_out.shape],
        [pltpu.SemaphoreType.DMA],
    )


def block_copies(c, blocks, hc, srcs, dsts, sems):
    copies = []
    for i, (mask, half) in enumerate(blocks):
        start = pl.multiple_of(((c ^ mask) * 2 + half) * hc, 16)
        for j in (0, 1):
            cp = pltpu.make_async_copy(
                srcs[j].at[:, pl.ds(start, hc), :],
                dsts[j].at[:, pl.ds(i * hc, hc), :],
                sems.at[i, j],
            )
            cp.start()
            copies.append(cp)
    return copies


def project(idx, hg, w_out, korder, emasks, tok):
    nctx = len(hg)
    rows, width = hg[0].shape
    total = nctx * rows
    cols = w_out.shape[1]

    def kernel(idx_ref, *refs):
        hg_ref = refs[:nctx]
        w_ref, send_ref, keep_ref = refs[nctx:]
        c = idx_ref[0]
        e = idx_ref[1]
        r = lax.broadcasted_iota(I32, (total, 1), 0)
        place = [0] * nctx
        for i, k in enumerate(korder):
            place[k] = i
        kp = jnp.zeros(r.shape, I32)
        rel = (r // tok) % nctx
        for k in range(nctx):
            kp = jnp.where(rel == (c ^ k), place[k], kp)
        j = pick(r // (nctx * tok), [e ^ m for m in emasks])
        src = kp * rows + j * tok + r % tok
        perm = (src == lax.broadcasted_iota(I32, (total, total), 1)).astype(F32).astype(BF)
        lhs = dot(perm, jnp.concatenate([h[...] for h in hg_ref], axis=0)).astype(BF)
        half = total // 2
        full = dot(lhs, w_ref[...])
        send_ref[...] = full[half:].astype(BF)
        keep_ref[...] = full[:half]

    return call(
        kernel,
        [((total // 2, cols), BF), ((total // 2, cols), F32)],
        (idx, *hg, held(w_out)),
        (pltpu.SMEM,) + (pltpu.VMEM,) * (nctx + 1),
        12,
        2 * total * width * cols,
    )


def choose(pairs):
    out = None
    for cond, x in pairs:
        x = jnp.where(cond, x, 0.0)
        out = x if out is None else out + x
    return out


def residual_parts(idx, residual, ids, nctx):
    tok, width = residual.shape
    cols = width // nctx
    top = ids.shape[1]

    def kernel(idx_ref, res_ref, ids_ref, *outs):
        c = idx_ref[0]
        lane = lax.broadcasted_iota(I32, (tok, EXTRA), 1)
        side = jnp.zeros((tok, EXTRA), F32)
        for t in range(top):
            side = jnp.where(lane - IDS == ids_ref[:, t : t + 1], 1.0, side)
        res = res_ref[...].astype(F32)
        for k in range(nctx):
            outs[k][:, :cols] = choose(
                [((c ^ k) == j, res[:, j * cols : (j + 1) * cols]) for j in range(nctx)]
            ).astype(BF)
            outs[k][:, cols:] = side.astype(BF)

    return call(
        kernel,
        [((tok, cols + EXTRA), BF)] * nctx,
        (idx, residual, ids),
        (pltpu.SMEM, pltpu.VMEM, pltpu.VMEM),
        4,
        1 << 28,
    )


def one_hot_rows(out_rows, in_rows, tok, shift):
    r = lax.broadcasted_iota(I32, (out_rows, in_rows), 0)
    q = lax.broadcasted_iota(I32, (out_rows, in_rows), 1)
    return ((r == q + shift * tok)).astype(F32).astype(BF)


def merge(idx, parts, own, got, gain, tok):
    nctx = len(parts)
    blk, cols = own.shape
    n = len(got)

    def kernel(idx_ref, *refs):
        c = idx_ref[0]
        prefs = refs[:nctx]
        own_ref = refs[nctx]
        grefs = refs[nctx + 1 : nctx + 1 + n]
        gain_ref, sx_ref, att_ref = refs[nctx + 1 + n :]
        att = own_ref[...]
        for g in grefs:
            att = att + g[...].astype(F32)
        att = att.astype(BF)
        att_ref[...] = att
        res = None
        for k in range(nctx):
            part = dot(one_hot_rows(blk, tok, tok, c ^ k), prefs[k][...])
            res = part if res is None else res + part
        hidden = res[:, :cols] + att.astype(F32)
        ssq = jnp.sum(hidden * hidden, axis=1, keepdims=True)
        gain = choose(
            [(c == j, gain_ref[:, j * cols : (j + 1) * cols]) for j in range(nctx)]
        )
        scaled = hidden * gain
        hi = ssq.astype(BF).astype(F32)
        mid = (ssq - hi).astype(BF).astype(F32)
        low = ssq - hi - mid
        extra = res[:, cols:]
        lane = lax.broadcasted_iota(I32, extra.shape, 1)
        extra = jnp.where(lane == 0, hi, jnp.where(lane == 1, mid, extra))
        extra = jnp.where(lane == 2, low, extra)
        sx_ref[:, :cols] = scaled.astype(BF)
        sx_ref[:, cols:] = extra.astype(BF)

    return call(
        kernel,
        [((blk, cols + EXTRA), BF), ((blk, cols), BF)],
        (idx, *parts, own, *got, gain),
        (pltpu.SMEM,) + (pltpu.VMEM,) * (nctx + n + 2),
        4,
        1 << 28,
    )


def attention_parts(idx, att, nctx, tok):
    cols = att.shape[1]

    def kernel(idx_ref, att_ref, *outs):
        c = idx_ref[0]
        r = lax.broadcasted_iota(I32, (tok, nctx * tok), 0)
        q = lax.broadcasted_iota(I32, (tok, nctx * tok), 1)
        for k in range(nctx):
            pickr = (q == r + (c ^ k) * tok).astype(F32).astype(BF)
            outs[k][...] = dot(pickr, att_ref[...]).astype(BF)

    return call(
        kernel,
        [((tok, cols), BF)] * nctx,
        (idx, att),
        (pltpu.SMEM, pltpu.VMEM),
        4,
        1 << 28,
    )


def finalize(idx, residual, parts, own, got):
    nctx = len(parts)
    tok, width = residual.shape
    cols = width // nctx
    n = len(got)

    def kernel(idx_ref, res_ref, *refs):
        c = idx_ref[0]
        prefs = [p[...].astype(F32) for p in refs[:nctx]]
        own_ref = refs[nctx]
        grefs = refs[nctx + 1 : nctx + 1 + n]
        out_ref = refs[nctx + 1 + n]
        for j in range(nctx):
            a, b = j * cols, (j + 1) * cols
            att = choose([((c ^ k) == j, prefs[k]) for k in range(nctx)])
            mix = own_ref[:, a:b]
            for g in grefs:
                mix = mix + g[:, a:b].astype(F32)
            out_ref[:, a:b] = (res_ref[:, a:b].astype(F32) + att + mix).astype(BF)

    return call(
        kernel,
        [((tok, width), BF)],
        (idx, residual, *parts, own, *got),
        (pltpu.SMEM,) + (pltpu.VMEM,) * (nctx + n + 2),
        4,
        1 << 28,
    )[0]


class Chunk:
    def __init__(self, pieces, mask, half):
        self.pieces = pieces
        self.mask = mask
        self.half = half


def grab(arrays, first=0, rows=None):
    n = len(arrays)
    shapes = [(rows or a.shape[0],) + a.shape[1:] for a in arrays]

    def kernel(*refs):
        sems = refs[2 * n]
        copies = []
        for i in range(n):
            src = refs[i].at[pl.ds(first, rows)] if rows else refs[i]
            copies.append(pltpu.make_async_copy(src, refs[n + i], sems.at[i]))
            copies[-1].start()
        for cp in copies:
            cp.wait()

    return call(
        kernel,
        [],
        tuple(arrays),
        (pltpu.HBM,) * n,
        1,
        1 << 30,
        shapes,
        [pltpu.SemaphoreType.DMA((n,))],
    )


def fetch(idx, blocks, w_gate, w_up, hc):
    local, _, ff = w_gate.shape
    n = len(blocks)

    def kernel(idx_ref, wg_ref, wu_ref, g_ref, u_ref, sems):
        srcs = (wg_ref, wu_ref)
        for cp in block_copies(idx_ref[0], blocks, hc, srcs, (g_ref, u_ref), sems):
            cp.wait()

    shape = (local, n * hc, ff)
    return call(
        kernel,
        [],
        (idx, w_gate, w_up),
        (pltpu.SMEM, pltpu.HBM, pltpu.HBM),
        1,
        1 << 30,
        [shape, shape],
        [pltpu.SemaphoreType.DMA((n, 2))],
    )


def experts(idx, chunks, router, groups, width, carry, finish, copy=None):
    loaded = [held(w) for g in groups for w in g[1:]]
    sizes = [len(g[0]) for g in groups]
    assert [b for g in groups for b in g[0]] == [(ch.mask, ch.half) for ch in chunks]
    local, _, ff = loaded[0].shape
    hc = router.shape[2]
    nw = len(loaded)
    pieces = [p for ch in chunks for p in ch.pieces]
    total = sum(p.shape[0] for p in chunks[0].pieces)
    nexperts = router.shape[1]
    n = len(pieces)
    ncarry = len(carry)

    def kernel(*refs):
        idx_ref = refs[0]
        prefs = refs[1 : 1 + n]
        r_ref = refs[1 + n]
        wrefs = refs[2 + n : 2 + n + nw]
        crefs = refs[2 + n + nw : 2 + n + nw + ncarry]
        outs = refs[2 + n + nw + ncarry :]
        if copy:
            wd_hbm, *outs, wd_ref, sem = outs
            src = wd_hbm.at[pl.ds(copy[1], copy[2])]
            load = pltpu.make_async_copy(src, wd_ref, sem)
            load.start()
        c = idx_ref[0]
        xs = []
        at = 0
        logit = crefs[2][...] if ncarry else jnp.zeros((total, nexperts), F32)
        ssum = crefs[3][...] if ncarry else jnp.zeros((total, 1), F32)
        for ch in chunks:
            parts = [prefs[at + i][...] for i in range(len(ch.pieces))]
            at += len(parts)
            x = parts[0] if len(parts) == 1 else jnp.concatenate(parts, axis=0)
            block = (c ^ ch.mask) * 2 + ch.half
            if ch.half == 1:
                extra = x[:, hc : hc + EXTRA].astype(F32)
                lane = lax.broadcasted_iota(I32, extra.shape, 1)
                ssum = ssum + jnp.sum(jnp.where(lane < 3, extra, 0.0), axis=1, keepdims=True)
                chosen = extra[:, IDS : IDS + nexperts]
            x = x[:, :hc]
            xs.append(x)
            logit = logit + dot_t(x, r_ref[block])
        pairs = []
        at = 0
        for g, size in enumerate(sizes):
            part = xs[at : at + size]
            at += size
            if hc % 128 == 0 and size > 1:
                pairs.append((jnp.concatenate(part, axis=1), g, 0, size * hc))
            else:
                pairs += [(x, g, i * hc, hc) for i, x in enumerate(part)]

        def product(e, c_i):
            acc = crefs[c_i][e] if ncarry else None
            for x, g, lo, size in pairs:
                part = dot(x, wrefs[2 * g + c_i][e, lo : lo + size, :])
                acc = part if acc is None else acc + part
            return acc

        if finish is None:
            for e in range(local):
                for c_i in (0, 1):
                    outs[c_i][e] = product(e, c_i)
            outs[2][...] = logit
            outs[3][...] = ssum
            return
        scale = lax.rsqrt(ssum / width + NORM_EPS)
        affinity = jax.nn.sigmoid(logit * scale) * chosen
        mixing = ROUTE_SCALE * affinity / jnp.sum(affinity, axis=1, keepdims=True)
        lane = lax.broadcasted_iota(I32, mixing.shape, 1)
        acts = []
        for e in range(local):
            vals = [product(e, c_i) * scale for c_i in (0, 1)]
            mine = idx_ref[1] * local + e
            mix = jnp.sum(jnp.where(lane == mine, mixing, 0.0), axis=1, keepdims=True)
            acts.append((jax.nn.silu(vals[0]) * vals[1] * mix).astype(BF))
        act = jnp.concatenate(acts, axis=1)
        nctx, tok, order_in, plan = finish
        r = lax.broadcasted_iota(I32, (total, 1), 0)
        pos = r // tok
        cm = pick(pos, [a for a, _ in plan])
        p = pick(pos, [order_in.index(b) for _, b in plan])
        src = (p * nctx + (c ^ cm)) * tok + r % tok
        perm = (src == lax.broadcasted_iota(I32, (total, total), 1)).astype(F32).astype(BF)
        outs[0][...] = dot(perm, act).astype(BF)
        if copy:
            load.wait()

    acc_shape = (local, total, ff)
    if finish is None:
        outs = [(acc_shape, F32), (acc_shape, F32), ((total, nexperts), F32), ((total, 1), F32)]
    else:
        outs = [((total, local * ff), BF)]
    args = (idx, *pieces, router, *loaded, *carry)
    specs = (pltpu.SMEM,) + (pltpu.VMEM,) * (len(args) - 1)
    flops = len(chunks) * 4 * total * hc * ff * local
    loads, scratch = [], []
    if copy:
        args += (copy[0],)
        specs += (pltpu.HBM,)
        loads = [(copy[2], width)]
        scratch = [pltpu.SemaphoreType.DMA]
    return call(kernel, outs, args, specs, 8, flops, loads, scratch)


def project_down(lhs, blocks, rows, lo, hi):
    total, depth = lhs.shape
    nr = len(rows)
    size = total // len(blocks)

    def kernel(x_ref, *refs):
        send_ref, keep_ref = refs[nr:]
        half = total // 2
        x = jnp.concatenate([x_ref[b * size : (b + 1) * size] for b in blocks], axis=0)
        for at in range(lo, hi, 1024):
            end = min(at + 1024, hi)
            acc = None
            k = 0
            for r in range(nr):
                n = rows[r].shape[0]
                part = dot(x[:, k : k + n], refs[r][:, at:end])
                k += n
                acc = part if acc is None else acc + part
            send_ref[:, at - lo : end - lo] = acc[half:].astype(BF)
            keep_ref[:, at - lo : end - lo] = acc[:half]

    return call(
        kernel,
        [((total // 2, hi - lo), BF), ((total // 2, hi - lo), F32)],
        (lhs, *[held(r) for r in rows]),
        (pltpu.VMEM,) * (nr + 1),
        8,
        2 * total * depth * (hi - lo),
    )


def body(
    q_nope,
    q_rope,
    cache_keys,
    fresh_keys,
    block_order,
    w_uv,
    w_out,
    residual,
    norm_gain,
    router_weight,
    expert_ids,
    w_gate,
    w_up,
    w_down,
):
    nctx = lax.axis_size("ctx")
    nexp = lax.axis_size("exp")
    c = lax.axis_index("ctx")
    e = lax.axis_index("exp")
    idx = jnp.stack([c, e]).astype(I32)
    cmasks = bits_of(nctx)
    emasks = bits_of(nexp)
    core, xs = cmasks[0], cmasks[1:]
    ym, zs = emasks[0], emasks[1:]
    zsub = subsets(zs)
    eorder = [y ^ z for y in (0, ym) for z in zsub]

    def swap(x, cm=0, em=0):
        m = cm * nexp + em
        return lax.ppermute(x, ("ctx", "exp"), [(i, i ^ m) for i in range(nctx * nexp)])

    rows_here, heads_here, lat = q_nope.shape
    tok, width = residual.shape
    cols = w_out.shape[1]
    hc = cols // 2
    total_rows = nctx * rows_here
    nexperts = router_weight.shape[1]
    block_rows = total_rows // block_order.shape[0]
    pe = q_rope.shape[1] // heads_here

    def spread(group):
        sets = [[x] for x in group]
        for m in xs:
            sets = [got + [swap(g, cm=m) for g in got] for got in sets]
        return [got + [swap(g, cm=core) for g in got] for got in sets]

    korder = subsets(xs)
    korder = korder + [k ^ core for k in korder]

    kf_own = fresh_keys.T
    kc_v, kf_v, w_uv_v = grab((cache_keys, kf_own, w_uv))
    q = q_nope.transpose(1, 0, 2).reshape(heads_here * rows_here, lat)
    qr = q_rope.reshape(rows_here, heads_here, pe).transpose(1, 0, 2)
    qr = qr.reshape(heads_here * rows_here, pe)
    meta = jnp.concatenate([idx, block_order])
    kc, kf = spread((cache_keys, kf_own))
    kc[0], kf[0] = held(kc_v), held(kf_v)
    head, w_out_v = attend(meta, q, qr, kc, kf, w_uv_v, w_out, korder, block_rows)

    xorder = subsets(xs)
    nx = len(xorder)
    blocks_1 = [(0, 0)]
    blocks_2 = [(m, 0) for m in xorder[1:]] + [(m, 1) for m in xorder]
    blocks_3 = [(m ^ core, h) for m, h in blocks_1 + blocks_2]

    def load(blocks):
        return (blocks, *fetch(idx, blocks, w_gate, w_up, hc))

    cut = len(blocks_2) * 2 // 3
    quarter = len(blocks_3) // 4
    groups_1 = [load(blocks_1)]
    groups_2 = [load(blocks_2[:cut]), load(blocks_2[cut:])]
    groups_3 = [load(blocks_3[: 2 * quarter])]
    groups_3 += [load(blocks_3[2 * quarter :])]
    w_down = w_down.reshape(-1, width)
    dq = w_down.shape[0] // 4
    down_v = grab((w_down,), 0, dq)
    down_v += grab((w_down,), dq, 2 * dq)

    res_got = residual_parts(idx, residual, expert_ids, nctx)
    res_got = [swap(p, cm=k) if k else p for k, p in enumerate(res_got)]

    (hg,) = spread((head,))
    send, keep = project(idx, hg, w_out_v, korder, eorder, tok)

    summed = keep + swap(send, em=ym).astype(F32)
    blk = nctx * tok
    got = [
        swap(summed[i * blk : (i + 1) * blk].astype(BF), em=m)
        for i, m in enumerate(zsub)
        if m
    ]
    sx, att_blk = merge(idx, res_got, summed[:blk], got, norm_gain[None], tok)

    zx = jnp.stack([swap(sx, em=m) if m else sx for m in zsub])
    zx = zx.reshape(len(zsub) * blk, -1)
    za = zx[:, :hc][None]
    zb = zx[:, hc:][None]
    own_a = jnp.concatenate([za, swap(za, em=ym)], axis=1)
    xb = zb
    for m in xs:
        xb = jnp.concatenate([xb, swap(xb, cm=m)], axis=0)
    far_b = swap(xb, em=ym)
    xa = own_a
    for m in xs:
        xa = jnp.concatenate([xa, swap(xa, cm=m)], axis=0)
    own_a_core = swap(own_a, cm=core)
    xb_core = swap(xb, cm=core)
    rest_a = xa[1:]
    rest_a_core = swap(rest_a, cm=core)
    far_b_core = swap(far_b, cm=core)

    router = router_weight.reshape(2 * nctx, hc, nexperts).transpose(0, 2, 1)
    first = [Chunk([own_a[0]], 0, 0)]
    g1 = experts(idx, first, router, groups_1, width, (), None)
    second = [Chunk([rest_a[i - 1]], xorder[i], 0) for i in range(1, nx)]
    second += [Chunk([xb[i], far_b[i]], xorder[i], 1) for i in range(nx)]
    g2 = experts(idx, second, router, groups_2, width, g1, None)
    third = [Chunk([own_a_core[0]], core, 0)]
    third += [Chunk([rest_a_core[i - 1]], core ^ xorder[i], 0) for i in range(1, nx)]
    third += [Chunk([xb_core[i], far_b_core[i]], core ^ xorder[i], 1) for i in range(nx)]

    xsub = subsets(xs)
    plan_a = [
        (k ^ x, y ^ z) for k in (0, core) for x in xsub for y in (0, ym) for z in zsub
    ]
    size_x = len(xsub)
    blocks_a = list(range(4 * size_x))
    blocks_b = [(k * size_x + x) * 2 + y for k in (0, 1) for y in (0, 1) for x in range(size_x)]
    steps_a = [(m, 0) for m in reversed(xs)] + [(0, ym)]
    steps_b = [(0, ym)] + [(m, 0) for m in reversed(xs)]
    finish = (nctx, tok, eorder, plan_a)
    last = (w_down, 3 * dq, dq)
    lhs, down_2 = experts(idx, third, router, groups_3, width, g2, finish, last)
    down_v.append(down_2)

    outs = []
    hw = width // 2
    halves = ((blocks_a, 0, hw, steps_a), (blocks_b, hw, width, steps_b))
    for blocks, lo, hi, steps in halves:
        send, keep = project_down(lhs, blocks, down_v, lo, hi)
        x = keep + swap(send, cm=core).astype(F32)
        for cm, em in steps:
            half = x.shape[0] // 2
            got = swap(x[half:].astype(BF), cm=cm, em=em)
            x = x[:half] + got.astype(F32)
        outs.append(x)

    parts = attention_parts(idx, att_blk, nctx, tok)
    parts = [swap(p, cm=k) if k else p for k, p in enumerate(parts)]

    both = jnp.concatenate(outs, axis=1)
    got = [
        swap(both[i * tok : (i + 1) * tok].astype(BF), em=m)
        for i, m in enumerate(zsub)
        if m
    ]
    return finalize(idx, residual, parts, both[:tok], got)


def solution(mesh):
    return jax.shard_map(
        body,
        mesh=mesh,
        in_specs=(
            P("ctx", "exp", None),
            P("ctx", "exp"),
            P(None, "ctx"),
            P(None, "ctx"),
            P(),
            P("exp", None, None),
            P("exp", "ctx"),
            P(("ctx", "exp"), None),
            P(),
            P(),
            P(("ctx", "exp"), None),
            P("exp", None, "ctx"),
            P("exp", None, "ctx"),
            P("exp", "ctx", None),
        ),
        out_specs=P(("ctx", "exp"), None),
        check_vma=False,
    )
```

```python
import math

import jax
import jax.numpy as jnp
from jax import lax
from jax.experimental import pallas as pl
from jax.experimental.pallas import tpu as pltpu
from jax.sharding import PartitionSpec as P


QKD = 192
ROUTE_SCALE = 2.5
NORM_EPS = 1e-06
EXTRA = 128
IDS = 16
GROUP_ROWS = 128
BF = jnp.bfloat16
F32 = jnp.float32
I32 = jnp.int32
NT = (((1,), (1,)), ((), ()))


def bits_of(count):
    masks = []
    bit = 1
    while bit < count:
        masks.append(bit)
        bit *= 2
    return masks


def subsets(masks):
    out = [0]
    for m in masks:
        out = out + [s | m for s in out]
    return out


def held(x):
    return pltpu.with_memory_space_constraint(x, pltpu.VMEM)


def dot(a, b):
    return jnp.dot(a, b, preferred_element_type=F32)


def dot_t(a, b):
    return lax.dot_general(a, b, NT, preferred_element_type=F32)


def call(kernel, outs, args, specs, limit, flops, loads=(), scratch=()):
    shapes = [jax.ShapeDtypeStruct(s, d) for s, d in outs]
    shapes += [pltpu.VMEM(s, BF) for s in loads]
    args = [
        pltpu.with_memory_space_constraint(a, pltpu.HBM) if s == pltpu.HBM else a
        for a, s in zip(args, specs)
    ]
    got = pl.pallas_call(
        kernel,
        out_shape=tuple(shapes),
        in_specs=[pl.BlockSpec(memory_space=s) for s in specs],
        out_specs=tuple(pl.BlockSpec(memory_space=pltpu.VMEM) for _ in shapes),
        scratch_shapes=list(scratch),
        compiler_params=pltpu.CompilerParams(vmem_limit_bytes=limit << 20),
        cost_estimate=pl.CostEstimate(flops=flops, bytes_accessed=0, transcendentals=0),
    )(*args)
    return list(got)


def pick(index, table):
    out = jnp.zeros(index.shape, I32)
    for i, v in enumerate(table):
        out = jnp.where(index == i, v, out)
    return out


def attend(meta, q, qr, kc, kf, w_uv, w_out, korder, block_rows):
    nctx = len(kc)
    kd, cache_len = kc[0].shape
    rows = kf[0].shape[0]
    heads, lat, vh = w_uv.shape
    group = max(1, min(heads, GROUP_ROWS // rows))
    nblk = meta.shape[0] - 2

    def kernel(*refs):
        idx_ref, q_ref, qr_ref = refs[:3]
        kc_ref = refs[3 : 3 + nctx]
        kf_ref = refs[3 + nctx : 3 + 2 * nctx]
        w_ref, wo_hbm, out_ref, wo_ref, sem = refs[3 + 2 * nctx :]
        load = pltpu.make_async_copy(wo_hbm, wo_ref, sem)
        load.start()
        c = idx_ref[0]
        starts = [idx_ref[2 + b] * block_rows for b in range(nblk)]

        def position(grow):
            return pick(grow // block_rows, starts) + grow % block_rows

        kfa = jnp.concatenate([k[...] for k in kf_ref], axis=0)
        kca = jnp.concatenate([k[...] for k in kc_ref], axis=1)
        col = lax.broadcasted_iota(I32, (1, nctx * rows), 1)
        owner = pick(col // rows, [c ^ k for k in korder])
        kpos = position(owner * rows + col % rows)
        row = lax.broadcasted_iota(I32, (group * rows, 1), 0)
        qpos = position(c * rows + row % rows)
        visible = kpos <= qpos
        scale = 1.0 / math.sqrt(QKD)
        for g in range(heads // group):
            lo = g * group * rows
            qb = q_ref[lo : lo + group * rows, :]
            rb = qr_ref[lo : lo + group * rows, :]
            sc = (dot(qb, kca[:lat]) + dot(rb, kca[lat:])) * scale
            sf = (dot_t(qb, kfa[:, :lat]) + dot_t(rb, kfa[:, lat:])) * scale
            sf = jnp.where(visible, sf, -jnp.inf)
            top = jnp.maximum(
                jnp.max(sc, axis=1, keepdims=True), jnp.max(sf, axis=1, keepdims=True)
            )
            pc = jnp.exp(sc - top)
            pf = jnp.exp(sf - top)
            total = jnp.sum(pc, axis=1, keepdims=True) + jnp.sum(pf, axis=1, keepdims=True)
            acc = dot_t(pc.astype(BF), kca[:lat]) + dot(pf.astype(BF), kfa[:, :lat])
            acc = acc / total
            hi = acc.astype(BF)
            low = (acc - hi.astype(F32)).astype(BF)
            for h in range(group):
                w = w_ref[g * group + h]
                a = h * rows
                v = dot(hi[a : a + rows], w) + dot(low[a : a + rows], w)
                n = (g * group + h) * vh
                out_ref[:, n : n + vh] = v.astype(BF)
        load.wait()

    specs = (pltpu.SMEM,) + (pltpu.VMEM,) * (3 + 2 * nctx) + (pltpu.HBM,)
    flops = 2 * heads * rows * nctx * (cache_len + rows) * (kd + lat)
    return call(
        kernel,
        [((rows, heads * vh), BF)],
        (meta, q, qr, *kc, *kf, held(w_uv), w_out),
        specs,
        16,
        flops,
        [w_out.shape],
        [pltpu.SemaphoreType.DMA],
    )


def block_copies(c, blocks, hc, srcs, dsts, sems):
    copies = []
    for i, (mask, half) in enumerate(blocks):
        start = pl.multiple_of(((c ^ mask) * 2 + half) * hc, 16)
        for j in (0, 1):
            cp = pltpu.make_async_copy(
                srcs[j].at[:, pl.ds(start, hc), :],
                dsts[j].at[:, pl.ds(i * hc, hc), :],
                sems.at[i, j],
            )
            cp.start()
            copies.append(cp)
    return copies


def project(idx, hg, w_out, korder, emasks, tok):
    nctx = len(hg)
    rows, width = hg[0].shape
    total = nctx * rows
    cols = w_out.shape[1]

    def kernel(idx_ref, *refs):
        hg_ref = refs[:nctx]
        w_ref, send_ref, keep_ref = refs[nctx:]
        c = idx_ref[0]
        e = idx_ref[1]
        r = lax.broadcasted_iota(I32, (total, 1), 0)
        place = [0] * nctx
        for i, k in enumerate(korder):
            place[k] = i
        kp = jnp.zeros(r.shape, I32)
        rel = (r // tok) % nctx
        for k in range(nctx):
            kp = jnp.where(rel == (c ^ k), place[k], kp)
        j = pick(r // (nctx * tok), [e ^ m for m in emasks])
        src = kp * rows + j * tok + r % tok
        perm = (src == lax.broadcasted_iota(I32, (total, total), 1)).astype(F32).astype(BF)
        lhs = dot(perm, jnp.concatenate([h[...] for h in hg_ref], axis=0)).astype(BF)
        half = total // 2
        full = dot(lhs, w_ref[...])
        send_ref[...] = full[half:].astype(BF)
        keep_ref[...] = full[:half]

    return call(
        kernel,
        [((total // 2, cols), BF), ((total // 2, cols), F32)],
        (idx, *hg, held(w_out)),
        (pltpu.SMEM,) + (pltpu.VMEM,) * (nctx + 1),
        12,
        2 * total * width * cols,
    )


def choose(pairs):
    out = None
    for cond, x in pairs:
        x = jnp.where(cond, x, 0.0)
        out = x if out is None else out + x
    return out


def residual_parts(idx, residual, ids, nctx):
    tok, width = residual.shape
    cols = width // nctx
    top = ids.shape[1]

    def kernel(idx_ref, res_ref, ids_ref, *outs):
        c = idx_ref[0]
        lane = lax.broadcasted_iota(I32, (tok, EXTRA), 1)
        side = jnp.zeros((tok, EXTRA), F32)
        for t in range(top):
            side = jnp.where(lane - IDS == ids_ref[:, t : t + 1], 1.0, side)
        res = res_ref[...].astype(F32)
        for k in range(nctx):
            outs[k][:, :cols] = choose(
                [((c ^ k) == j, res[:, j * cols : (j + 1) * cols]) for j in range(nctx)]
            ).astype(BF)
            outs[k][:, cols:] = side.astype(BF)

    return call(
        kernel,
        [((tok, cols + EXTRA), BF)] * nctx,
        (idx, residual, ids),
        (pltpu.SMEM, pltpu.VMEM, pltpu.VMEM),
        4,
        1 << 28,
    )


def one_hot_rows(out_rows, in_rows, tok, shift):
    r = lax.broadcasted_iota(I32, (out_rows, in_rows), 0)
    q = lax.broadcasted_iota(I32, (out_rows, in_rows), 1)
    return ((r == q + shift * tok)).astype(F32).astype(BF)


def place_rows(idx, parts, gain, blk, tok):
    nctx = len(parts)
    wide = parts[0].shape[1]
    cols = wide - EXTRA

    def kernel(idx_ref, *refs):
        c = idx_ref[0]
        gain_ref, res_ref, row_ref = refs[nctx:]
        res = None
        for k in range(nctx):
            part = dot(one_hot_rows(blk, tok, tok, c ^ k), refs[k][...])
            res = part if res is None else res + part
        res_ref[...] = res
        row_ref[...] = choose(
            [(c == j, gain_ref[:, j * cols : (j + 1) * cols]) for j in range(nctx)]
        )

    return call(
        kernel,
        [((blk, wide), F32), ((1, cols), F32)],
        (idx, *parts, gain),
        (pltpu.SMEM,) + (pltpu.VMEM,) * (nctx + 1),
        4,
        1 << 28,
    )


def merge(res, gain, own, got):
    blk, cols = own.shape
    n = len(got)

    def kernel(res_ref, gain_ref, own_ref, *refs):
        sx_ref, att_ref = refs[n:]
        att = own_ref[...]
        for g in refs[:n]:
            att = att + g[...].astype(F32)
        att = att.astype(BF)
        att_ref[...] = att
        hidden = res_ref[:, :cols] + att.astype(F32)
        ssq = jnp.sum(hidden * hidden, axis=1, keepdims=True)
        hi = ssq.astype(BF).astype(F32)
        mid = (ssq - hi).astype(BF).astype(F32)
        low = ssq - hi - mid
        extra = res_ref[:, cols:]
        lane = lax.broadcasted_iota(I32, extra.shape, 1)
        extra = jnp.where(lane == 0, hi, jnp.where(lane == 1, mid, extra))
        extra = jnp.where(lane == 2, low, extra)
        sx_ref[:, :cols] = (hidden * gain_ref[...]).astype(BF)
        sx_ref[:, cols:] = extra.astype(BF)

    return call(
        kernel,
        [((blk, cols + EXTRA), BF), ((blk, cols), BF)],
        (res, gain, own, *got),
        (pltpu.VMEM,) * (n + 3),
        4,
        1 << 28,
    )


def attention_parts(idx, att, nctx, tok):
    cols = att.shape[1]

    def kernel(idx_ref, att_ref, *outs):
        c = idx_ref[0]
        r = lax.broadcasted_iota(I32, (tok, nctx * tok), 0)
        q = lax.broadcasted_iota(I32, (tok, nctx * tok), 1)
        for k in range(nctx):
            pickr = (q == r + (c ^ k) * tok).astype(F32).astype(BF)
            outs[k][...] = dot(pickr, att_ref[...]).astype(BF)

    return call(
        kernel,
        [((tok, cols), BF)] * nctx,
        (idx, att),
        (pltpu.SMEM, pltpu.VMEM),
        4,
        1 << 28,
    )


def finalize(idx, residual, parts, own, got):
    nctx = len(parts)
    tok, width = residual.shape
    cols = width // nctx
    n = len(got)

    def kernel(idx_ref, res_ref, *refs):
        c = idx_ref[0]
        prefs = [p[...].astype(F32) for p in refs[:nctx]]
        own_ref = refs[nctx]
        grefs = refs[nctx + 1 : nctx + 1 + n]
        out_ref = refs[nctx + 1 + n]
        for j in range(nctx):
            a, b = j * cols, (j + 1) * cols
            att = choose([((c ^ k) == j, prefs[k]) for k in range(nctx)])
            mix = own_ref[:, a:b]
            for g in grefs:
                mix = mix + g[:, a:b].astype(F32)
            out_ref[:, a:b] = (res_ref[:, a:b].astype(F32) + att + mix).astype(BF)

    return call(
        kernel,
        [((tok, width), BF)],
        (idx, residual, *parts, own, *got),
        (pltpu.SMEM,) + (pltpu.VMEM,) * (nctx + n + 2),
        4,
        1 << 28,
    )[0]


class Chunk:
    def __init__(self, pieces, mask, half):
        self.pieces = pieces
        self.mask = mask
        self.half = half


def grab(arrays, first=0, rows=None):
    n = len(arrays)
    shapes = [(rows or a.shape[0],) + a.shape[1:] for a in arrays]

    def kernel(*refs):
        sems = refs[2 * n]
        copies = []
        for i in range(n):
            src = refs[i].at[pl.ds(first, rows)] if rows else refs[i]
            copies.append(pltpu.make_async_copy(src, refs[n + i], sems.at[i]))
            copies[-1].start()
        for cp in copies:
            cp.wait()

    return call(
        kernel,
        [],
        tuple(arrays),
        (pltpu.HBM,) * n,
        1,
        1 << 30,
        shapes,
        [pltpu.SemaphoreType.DMA((n,))],
    )


def fetch(idx, blocks, w_gate, w_up, hc):
    local, _, ff = w_gate.shape
    n = len(blocks)

    def kernel(idx_ref, wg_ref, wu_ref, g_ref, u_ref, sems):
        srcs = (wg_ref, wu_ref)
        for cp in block_copies(idx_ref[0], blocks, hc, srcs, (g_ref, u_ref), sems):
            cp.wait()

    shape = (local, n * hc, ff)
    return call(
        kernel,
        [],
        (idx, w_gate, w_up),
        (pltpu.SMEM, pltpu.HBM, pltpu.HBM),
        1,
        1 << 30,
        [shape, shape],
        [pltpu.SemaphoreType.DMA((n, 2))],
    )


def experts(idx, chunks, router, groups, width, carry, finish, copy=None):
    loaded = [held(w) for g in groups for w in g[1:]]
    sizes = [len(g[0]) for g in groups]
    assert [b for g in groups for b in g[0]] == [(ch.mask, ch.half) for ch in chunks]
    local, _, ff = loaded[0].shape
    hc = router.shape[2]
    nw = len(loaded)
    pieces = [p for ch in chunks for p in ch.pieces]
    total = sum(p.shape[0] for p in chunks[0].pieces)
    nexperts = router.shape[1]
    n = len(pieces)
    ncarry = len(carry)

    def kernel(*refs):
        idx_ref = refs[0]
        prefs = refs[1 : 1 + n]
        r_ref = refs[1 + n]
        wrefs = refs[2 + n : 2 + n + nw]
        crefs = refs[2 + n + nw : 2 + n + nw + ncarry]
        outs = refs[2 + n + nw + ncarry :]
        if copy:
            wd_hbm, *outs, wd_ref, sem = outs
            src = wd_hbm.at[pl.ds(copy[1], copy[2])]
            load = pltpu.make_async_copy(src, wd_ref, sem)
            load.start()
        c = idx_ref[0]
        xs = []
        at = 0
        logit = crefs[2][...] if ncarry else jnp.zeros((total, nexperts), F32)
        ssum = crefs[3][...] if ncarry else jnp.zeros((total, 1), F32)
        for ch in chunks:
            parts = [prefs[at + i][...] for i in range(len(ch.pieces))]
            at += len(parts)
            x = parts[0] if len(parts) == 1 else jnp.concatenate(parts, axis=0)
            block = (c ^ ch.mask) * 2 + ch.half
            if ch.half == 1:
                extra = x[:, hc : hc + EXTRA].astype(F32)
                lane = lax.broadcasted_iota(I32, extra.shape, 1)
                ssum = ssum + jnp.sum(jnp.where(lane < 3, extra, 0.0), axis=1, keepdims=True)
                chosen = extra[:, IDS : IDS + nexperts]
            x = x[:, :hc]
            xs.append(x)
            logit = logit + dot_t(x, r_ref[block])
        pairs = []
        at = 0
        for g, size in enumerate(sizes):
            part = xs[at : at + size]
            at += size
            if hc % 128 == 0 and size > 1:
                pairs.append((jnp.concatenate(part, axis=1), g, 0, size * hc))
            else:
                pairs += [(x, g, i * hc, hc) for i, x in enumerate(part)]

        def product(e, c_i):
            acc = crefs[c_i][e] if ncarry else None
            for x, g, lo, size in pairs:
                part = dot(x, wrefs[2 * g + c_i][e, lo : lo + size, :])
                acc = part if acc is None else acc + part
            return acc

        if finish is None:
            for e in range(local):
                for c_i in (0, 1):
                    outs[c_i][e] = product(e, c_i)
            outs[2][...] = logit
            outs[3][...] = ssum
            if copy:
                load.wait()
            return
        scale = lax.rsqrt(ssum / width + NORM_EPS)
        affinity = jax.nn.sigmoid(logit * scale) * chosen
        mixing = ROUTE_SCALE * affinity / jnp.sum(affinity, axis=1, keepdims=True)
        lane = lax.broadcasted_iota(I32, mixing.shape, 1)
        acts = []
        for e in range(local):
            vals = [product(e, c_i) * scale for c_i in (0, 1)]
            mine = idx_ref[1] * local + e
            mix = jnp.sum(jnp.where(lane == mine, mixing, 0.0), axis=1, keepdims=True)
            acts.append((jax.nn.silu(vals[0]) * vals[1] * mix).astype(BF))
        act = jnp.concatenate(acts, axis=1)
        nctx, tok, order_in, plan = finish
        r = lax.broadcasted_iota(I32, (total, 1), 0)
        pos = r // tok
        cm = pick(pos, [a for a, _ in plan])
        p = pick(pos, [order_in.index(b) for _, b in plan])
        src = (p * nctx + (c ^ cm)) * tok + r % tok
        perm = (src == lax.broadcasted_iota(I32, (total, total), 1)).astype(F32).astype(BF)
        outs[0][...] = dot(perm, act).astype(BF)
        if copy:
            load.wait()

    acc_shape = (local, total, ff)
    if finish is None:
        outs = [(acc_shape, F32), (acc_shape, F32), ((total, nexperts), F32), ((total, 1), F32)]
    else:
        outs = [((total, local * ff), BF)]
    args = (idx, *pieces, router, *loaded, *carry)
    specs = (pltpu.SMEM,) + (pltpu.VMEM,) * (len(args) - 1)
    flops = len(chunks) * 4 * total * hc * ff * local
    loads, scratch = [], []
    if copy:
        args += (copy[0],)
        specs += (pltpu.HBM,)
        loads = [(copy[2], width)]
        scratch = [pltpu.SemaphoreType.DMA]
    return call(kernel, outs, args, specs, 8, flops, loads, scratch)


def project_down(lhs, blocks, rows, lo, hi):
    total, depth = lhs.shape
    nr = len(rows)
    size = total // len(blocks)

    def kernel(x_ref, *refs):
        send_ref, keep_ref = refs[nr:]
        half = total // 2
        x = jnp.concatenate([x_ref[b * size : (b + 1) * size] for b in blocks], axis=0)
        for at in range(lo, hi, 1024):
            end = min(at + 1024, hi)
            acc = None
            k = 0
            for r in range(nr):
                n = rows[r].shape[0]
                part = dot(x[:, k : k + n], refs[r][:, at:end])
                k += n
                acc = part if acc is None else acc + part
            send_ref[:, at - lo : end - lo] = acc[half:].astype(BF)
            keep_ref[:, at - lo : end - lo] = acc[:half]

    return call(
        kernel,
        [((total // 2, hi - lo), BF), ((total // 2, hi - lo), F32)],
        (lhs, *[held(r) for r in rows]),
        (pltpu.VMEM,) * (nr + 1),
        8,
        2 * total * depth * (hi - lo),
    )


def body(
    q_nope,
    q_rope,
    cache_keys,
    fresh_keys,
    block_order,
    w_uv,
    w_out,
    residual,
    norm_gain,
    router_weight,
    expert_ids,
    w_gate,
    w_up,
    w_down,
):
    nctx = lax.axis_size("ctx")
    nexp = lax.axis_size("exp")
    c = lax.axis_index("ctx")
    e = lax.axis_index("exp")
    idx = jnp.stack([c, e]).astype(I32)
    cmasks = bits_of(nctx)
    emasks = bits_of(nexp)
    core, xs = cmasks[0], cmasks[1:]
    ym, zs = emasks[0], emasks[1:]
    zsub = subsets(zs)
    eorder = [y ^ z for y in (0, ym) for z in zsub]

    def swap(x, cm=0, em=0):
        m = cm * nexp + em
        return lax.ppermute(x, ("ctx", "exp"), [(i, i ^ m) for i in range(nctx * nexp)])

    rows_here, heads_here, lat = q_nope.shape
    tok, width = residual.shape
    cols = w_out.shape[1]
    hc = cols // 2
    total_rows = nctx * rows_here
    nexperts = router_weight.shape[1]
    block_rows = total_rows // block_order.shape[0]
    pe = q_rope.shape[1] // heads_here

    def spread(group):
        sets = [[x] for x in group]
        for m in xs:
            sets = [got + [swap(g, cm=m) for g in got] for got in sets]
        return [got + [swap(g, cm=core) for g in got] for got in sets]

    korder = subsets(xs)
    korder = korder + [k ^ core for k in korder]

    kf_own = fresh_keys.T
    kc_v, kf_v, w_uv_v = grab((cache_keys, kf_own, w_uv))
    q = q_nope.transpose(1, 0, 2).reshape(heads_here * rows_here, lat)
    qr = q_rope.reshape(rows_here, heads_here, pe).transpose(1, 0, 2)
    qr = qr.reshape(heads_here * rows_here, pe)
    meta = jnp.concatenate([idx, block_order])
    kc, kf = spread((cache_keys, kf_own))
    kc[0], kf[0] = held(kc_v), held(kf_v)
    head, w_out_v = attend(meta, q, qr, kc, kf, w_uv_v, w_out, korder, block_rows)

    xorder = subsets(xs)
    nx = len(xorder)
    blocks_1 = [(0, 0)]
    blocks_2 = [(m, 0) for m in xorder[1:]] + [(m, 1) for m in xorder]
    blocks_3 = [(m ^ core, h) for m, h in blocks_1 + blocks_2]

    def load(blocks):
        return (blocks, *fetch(idx, blocks, w_gate, w_up, hc))

    cut = len(blocks_2) * 2 // 3
    quarter = len(blocks_3) // 4
    groups_1 = [load(blocks_1)]
    groups_2 = [load(blocks_2[:cut]), load(blocks_2[cut:])]
    groups_3 = [load(blocks_3[: 2 * quarter])]
    groups_3 += [load(blocks_3[2 * quarter :])]
    w_down = w_down.reshape(-1, width)
    dq = w_down.shape[0] // 4
    down_v = grab((w_down,), 0, dq)

    res_got = residual_parts(idx, residual, expert_ids, nctx)
    res_got = [swap(p, cm=k) if k else p for k, p in enumerate(res_got)]

    (hg,) = spread((head,))
    send, keep = project(idx, hg, w_out_v, korder, eorder, tok)

    summed = keep + swap(send, em=ym).astype(F32)
    blk = nctx * tok
    got = [
        swap(summed[i * blk : (i + 1) * blk].astype(BF), em=m)
        for i, m in enumerate(zsub)
        if m
    ]
    res_rows, gain_row = place_rows(idx, res_got, norm_gain[None], blk, tok)
    sx, att_blk = merge(res_rows, gain_row, summed[:blk], got)

    zx = jnp.stack([swap(sx, em=m) if m else sx for m in zsub])
    zx = zx.reshape(len(zsub) * blk, -1)
    za = zx[:, :hc][None]
    zb = zx[:, hc:][None]
    own_a = jnp.concatenate([za, swap(za, em=ym)], axis=1)
    xb = zb
    for m in xs:
        xb = jnp.concatenate([xb, swap(xb, cm=m)], axis=0)
    far_b = swap(xb, em=ym)
    xa = own_a
    for m in xs:
        xa = jnp.concatenate([xa, swap(xa, cm=m)], axis=0)
    own_a_core = swap(own_a, cm=core)
    xb_core = swap(xb, cm=core)
    rest_a = xa[1:]
    rest_a_core = swap(rest_a, cm=core)
    far_b_core = swap(far_b, cm=core)

    router = router_weight.reshape(2 * nctx, hc, nexperts).transpose(0, 2, 1)
    first = [Chunk([own_a[0]], 0, 0)]
    *g1, down_1 = experts(
        idx, first, router, groups_1, width, (), None, (w_down, dq, 2 * dq)
    )
    down_v.append(down_1)
    second = [Chunk([rest_a[i - 1]], xorder[i], 0) for i in range(1, nx)]
    second += [Chunk([xb[i], far_b[i]], xorder[i], 1) for i in range(nx)]
    g2 = experts(idx, second, router, groups_2, width, g1, None)
    third = [Chunk([own_a_core[0]], core, 0)]
    third += [Chunk([rest_a_core[i - 1]], core ^ xorder[i], 0) for i in range(1, nx)]
    third += [Chunk([xb_core[i], far_b_core[i]], core ^ xorder[i], 1) for i in range(nx)]

    xsub = subsets(xs)
    plan_a = [
        (k ^ x, y ^ z) for k in (0, core) for x in xsub for y in (0, ym) for z in zsub
    ]
    size_x = len(xsub)
    blocks_a = list(range(4 * size_x))
    blocks_b = [(k * size_x + x) * 2 + y for k in (0, 1) for y in (0, 1) for x in range(size_x)]
    steps_a = [(m, 0) for m in reversed(xs)] + [(0, ym)]
    steps_b = [(0, ym)] + [(m, 0) for m in reversed(xs)]
    finish = (nctx, tok, eorder, plan_a)
    last = (w_down, 3 * dq, dq)
    lhs, down_2 = experts(idx, third, router, groups_3, width, g2, finish, last)
    down_v.append(down_2)

    outs = []
    hw = width // 2
    halves = ((blocks_a, 0, hw, steps_a), (blocks_b, hw, width, steps_b))
    for blocks, lo, hi, steps in halves:
        send, keep = project_down(lhs, blocks, down_v, lo, hi)
        x = keep + swap(send, cm=core).astype(F32)
        for cm, em in steps:
            half = x.shape[0] // 2
            got = swap(x[half:].astype(BF), cm=cm, em=em)
            x = x[:half] + got.astype(F32)
        outs.append(x)

    parts = attention_parts(idx, att_blk, nctx, tok)
    parts = [swap(p, cm=k) if k else p for k, p in enumerate(parts)]

    both = jnp.concatenate(outs, axis=1)
    got = [
        swap(both[i * tok : (i + 1) * tok].astype(BF), em=m)
        for i, m in enumerate(zsub)
        if m
    ]
    return finalize(idx, residual, parts, both[:tok], got)


def solution(mesh):
    return jax.shard_map(
        body,
        mesh=mesh,
        in_specs=(
            P("ctx", "exp", None),
            P("ctx", "exp"),
            P(None, "ctx"),
            P(None, "ctx"),
            P(),
            P("exp", None, None),
            P("exp", "ctx"),
            P(("ctx", "exp"), None),
            P(),
            P(),
            P(("ctx", "exp"), None),
            P("exp", None, "ctx"),
            P("exp", None, "ctx"),
            P("exp", "ctx", None),
        ),
        out_specs=P(("ctx", "exp"), None),
        check_vma=False,
    )
```
